32 devices in a mesh: seq: 32 (over z, y, x, core).
Axes of the slice: x: 2, y: 2, z: 4, core: 2. Of those that a mesh axis runs over, the one named last changes fastest.
Arguments:
- queries: bfloat16 [2, 4, 128, 576], replicated, may hold values from -40 to 40
- latent_cache: bfloat16 [2, 131072, 576], P(None, 'seq'), may hold values from -6 to 6
- lengths: int32 [2], replicated, may hold values from 16384 to 131072
- offsets: int32 [2, 4], replicated, may hold values from 0 to 3
Outputs:
- attended: bfloat16 [2, 4, 128, 512], replicated
The draws below stay inside these ranges and needn't reach their ends.
All inputs are finite; a program needn't handle non-finite values.
Results may differ from the reference program's by a relative error of at most 0.001.
The reference program's roundings to bfloat16 on the way count: a program that leaves them out, or rounds other values in their place, can miss the bound.
Values may be sent and summed in bfloat16 or wider, within the bound.
A program may use at most 128 MiB of HBM per device.

```python
import jax
import jax.numpy as jnp
from jax import lax

HEADS = 128
LATENT = 512
ROPE = 64
QTOK = 4
REQS = 2
CACHE_DEV = 4096
SEQ = 131072
N_SEQ = 32


def special(key):
    base = jax.random.fold_in(key, 11)
    key_vec, key_noise, key_spot, key_strength = jax.random.split(base, 4)
    count = 2 * REQS
    width = LATENT + ROPE
    signs = jnp.where(jax.random.normal(key_vec, (count, width), jnp.float32) > 0.0, 2.0, -2.0)
    vectors = signs.astype(jnp.float32)
    noise = 0.5 * jax.random.normal(key_noise, (count, width), jnp.float32)
    along = jnp.sum(noise * vectors, axis=1, keepdims=True) / (4.0 * width)
    across = noise - along * vectors
    targets = 120.0 + 100.0 * jax.random.randint(key_strength, (count,), 0, 4).astype(jnp.float32)
    shrink = 1.0 - 2.0 / targets
    twins = jnp.clip(shrink[:, None] * vectors + across, -6.0, 6.0)
    strengths = targets / (4.0 * width * 192.0 ** (-0.5))
    stride = SEQ // 16
    spots = jnp.arange(count) // REQS * stride + jax.random.randint(key_spot, (count,), 0, stride - 8)
    return (vectors, twins, spots, strengths)


def draw_latent_cache(key, part):
    shape = (REQS, SEQ, LATENT + ROPE)
    cache = jax.random.normal(jax.random.fold_in(key, 3), shape, jnp.float32)
    vectors, twins, spots, strengths = special(key)
    owners = jnp.arange(2 * REQS) % REQS
    cache = cache.at[owners, spots].set(vectors)
    cache = cache.at[owners, spots + 1].set(twins)
    return jnp.clip(cache, -6.0, 6.0).astype(jnp.bfloat16)


def draw_queries(key, part):
    shape = (REQS, QTOK, HEADS, LATENT + ROPE)
    values = jnp.clip(jax.random.normal(jax.random.fold_in(key, 5), shape, jnp.float32), -6.0, 6.0)
    vectors, twins, spots, strengths = special(key)
    counter = jnp.arange(2 * REQS)
    owners = counter % REQS
    tokens = counter % QTOK
    chosen = counter * 7 % HEADS
    aligned = strengths[:, None] * vectors
    values = values.at[owners, tokens, chosen].set(jnp.clip(aligned, -40.0, 40.0))
    return values.astype(jnp.bfloat16)


def place_ends(array, rng, least, largest):
    shape = array.shape
    place = [jax.random.randint(jax.random.fold_in(rng, axis), (), 0, shape[axis]) for axis in range(len(shape))]
    array = array.at[tuple(place)].set(least)
    longest = shape.index(max(shape))
    place[longest] = (place[longest] + 1) % shape[longest]
    return array.at[tuple(place)].set(largest)


def setup_inputs(seed: int = 0) -> dict:
    splits = jax.random.split(jax.random.key(seed), 5)
    return {
        "queries": draw_queries(jax.random.fold_in(splits[4], 71), 0),
        "latent_cache": draw_latent_cache(jax.random.fold_in(splits[4], 71), 0),
        "lengths": jax.random.randint(splits[2], (REQS,), SEQ // 8, SEQ + 1).astype(jnp.int32),
        "offsets": place_ends(jax.random.randint(splits[3], (REQS, QTOK), 0, QTOK), jax.random.fold_in(splits[3], 1), 0, QTOK - 1).astype(jnp.int32),
    }


softmax_scale = 192.0 ** -0.5


def one_request(operands):
    query, cache, length, offset = operands
    rows = query.reshape(QTOK * HEADS, LATENT + ROPE)
    limit = jnp.repeat(length - QTOK + 1 + offset, HEADS)

    def block(index):
        keys = lax.dynamic_slice_in_dim(cache, (index * CACHE_DEV).astype(jnp.int32), CACHE_DEV, 0)
        score = jnp.dot(rows, keys.T, preferred_element_type=jnp.float32) * softmax_scale
        places = index * CACHE_DEV + jnp.arange(CACHE_DEV, dtype=jnp.int32)
        visible = places[None, :] < limit[:, None]
        score = jnp.where(visible, score, -1e30)
        peak = jnp.max(score, axis=1)
        weight = jnp.where(visible, jnp.exp(score - peak[:, None]), 0.0)
        total = jnp.sum(weight, axis=1)
        partial_value = jnp.dot(weight.astype(jnp.bfloat16), keys[:, :LATENT], preferred_element_type=jnp.float32)
        return peak, total, partial_value

    peaks, totals, partials = lax.map(block, jnp.arange(N_SEQ, dtype=jnp.int32))
    top = jnp.max(peaks, axis=0)
    factor = jnp.exp(peaks - top[None, :])
    upper = jnp.sum(factor[:, :, None] * partials, axis=0)
    lower = jnp.sum(factor * totals, axis=0)
    return (upper / lower[:, None]).astype(jnp.bfloat16).reshape(QTOK, HEADS, LATENT)


def reference(queries, latent_cache, lengths, offsets):
    return lax.map(one_request, (queries, latent_cache, lengths, offsets))
```

```python
import functools

import jax
import jax.numpy as jnp
from jax import lax
from jax.experimental import pallas as pl
from jax.experimental.pallas import tpu as pltpu
from jax.sharding import PartitionSpec as P

LATENT = 512
LANES = 128
LOG2E = 1.4426950408889634
SCALE2 = (192.0 ** (-0.5)) * LOG2E
MESH = pl.DeviceIdType.MESH


def plan(n):
    chips, radices = n // 2, []
    while chips > 1:
        radix = 4 if chips % 4 == 0 else 2
        radices.append(radix)
        chips //= radix
    return radices


def split_meta(block, half):
    return block[:, :half], block[:, half:half + 1], block[:, half + 64:half + 65]


def with_meta(ref_index, ref, value, peak, total, half):
    rows = value.shape[0]
    lane = lax.broadcasted_iota(jnp.int32, (rows, LANES), 1)
    ref[(*ref_index, slice(None), pl.ds(0, half))] = value
    ref[(*ref_index, slice(None), pl.ds(half, LANES))] = jnp.where(lane < 64, peak, total)


def combine(blocks, half):
    parts = [split_meta(block, half) for block in blocks]
    top = functools.reduce(jnp.maximum, [p[1] for p in parts])
    factors = [jnp.exp2(p[1] - top) for p in parts]
    value = sum(p[0] * f for p, f in zip(parts, factors))
    total = sum(p[2] * f for p, f in zip(parts, factors))
    return value, top, total


def kernel(n, qtok, heads, chunk, lengths, offsets, q_ref, cache_hbm, out_ref,
           kv, score, w0, core_in, works, stage_in, gathered, load_sem, send_sem, recv_sem):
    rows_all = q_ref.shape[0]
    cache_dev = kv.shape[1]
    half = LATENT // 2
    chunks = rows_all // chunk
    per_request = qtok * heads // chunk
    tokens = chunk // heads
    radices = plan(n)
    stages = len(radices)
    strides, blocks, pieces = [], [], n // 2
    stride, left = 1, pieces
    for radix in radices:
        strides.append(stride)
        stride *= radix
        left //= radix
        blocks.append(left)
    piece_rows = chunk // pieces

    me = lax.axis_index("seq")
    core = lax.rem(me, 2)
    chip = me // 2
    digits = [lax.rem(chip // s, r) for s, r in zip(strides, radices)]
    partner = me + 1 - 2 * core

    def peer(stage, d):
        other = lax.rem(digits[stage] + d, radices[stage])
        return other, me + (other - digits[stage]) * strides[stage] * 2

    barrier = pltpu.get_barrier_semaphore()
    peers = [partner]
    for stage in range(stages):
        peers += [peer(stage, d)[1] for d in range(1, radices[stage])]
    for device in peers:
        pl.semaphore_signal(barrier, inc=1, device_id=(device,), device_id_type=MESH)

    def load(b):
        return pltpu.make_async_copy(cache_hbm.at[b], kv.at[b], load_sem.at[b])

    load(0).start()
    pl.semaphore_wait(barrier, len(peers))

    start = me * cache_dev
    span = 512
    value_span = 1024

    def remote(src, dst, j, slot, device):
        return pltpu.make_async_remote_copy(
            src_ref=src, dst_ref=dst, send_sem=send_sem.at[j, slot],
            recv_sem=recv_sem.at[j, slot], device_id=(device,), device_id_type=MESH)

    def core_copy(j):
        return remote(w0.at[j, 1 - core], core_in.at[j], j, 0, partner)

    def stage_copy(j, stage, d):
        other, device = peer(stage, d)
        rows = chunk
        for r in radices[:stage + 1]:
            rows //= r
        src = works[stage].at[j, pl.ds(other * rows, rows)]
        return remote(src, stage_in[stage].at[j, d - 1], j, 1 + 3 * stage + d - 1, device)

    def first_piece(stage):
        return sum(digits[i] * blocks[i] for i in range(stage + 1))

    def gather_copy(j, stage, d):
        _, device = peer(stage, d)
        ref = gathered.at[j, core, pl.ds(first_piece(stage), blocks[stage])]
        return remote(ref, ref, j, 1 + 3 * stages + 3 * stage + d - 1, device)

    def gather_arrival(j, stage, d):
        _, device = peer(stage, d)
        origin = lax.rem(digits[stage] + radices[stage] - d, radices[stage])
        first = origin * blocks[stage]
        if stage:
            first = first + first_piece(stage - 1)
        ref = gathered.at[j, core, pl.ds(first, blocks[stage])]
        return remote(ref, ref, j, 1 + 3 * stages + 3 * stage + d - 1, device)

    def core_gather(j, which):
        ref = gathered.at[j, which]
        return remote(ref, ref, j, 1 + 6 * stages, partner)

    def compute(c):
        b = c // per_request
        first_token = lax.rem(c, per_request) * tokens
        limits = [lengths[b] - (qtok - 1) + offsets[b, first_token + t] - start for t in range(tokens)]
        q = q_ref[pl.ds(pl.multiple_of(c * chunk, chunk), chunk), :]
        peak = jnp.full((chunk, LANES), -1e30, jnp.float32)
        for j in range(cache_dev // span):
            s = lax.dot_general(q, kv[b, j * span:(j + 1) * span, :], (((1,), (1,)), ((), ())),
                                preferred_element_type=jnp.float32)
            places = lax.broadcasted_iota(jnp.int32, (heads, span), 1) + j * span
            s = jnp.concatenate(
                [jnp.where(places < limits[t], s[t * heads:(t + 1) * heads] * SCALE2, -1e30)
                 for t in range(tokens)], axis=0)
            score[:, j * span:(j + 1) * span] = s
            for i in range(span // LANES):
                peak = jnp.maximum(peak, s[:, i * LANES:(i + 1) * LANES])
        peak = jnp.max(peak, axis=1, keepdims=True)
        base = jnp.maximum(peak, -1e29)
        total = jnp.zeros((chunk, LANES), jnp.float32)
        value = jnp.zeros((chunk, LATENT), jnp.float32)
        for j in range(cache_dev // value_span):
            w = jnp.exp2(score[:, j * value_span:(j + 1) * value_span] - base)
            for i in range(value_span // LANES):
                total = total + w[:, i * LANES:(i + 1) * LANES]
            value = value + jnp.dot(w.astype(jnp.bfloat16),
                                    kv[b, j * value_span:(j + 1) * value_span, :LATENT],
                                    preferred_element_type=jnp.float32)
        total = jnp.sum(total, axis=1, keepdims=True)
        for h in range(2):
            with_meta((c, h), w0, value[:, h * half:(h + 1) * half], peak, total, half)
        core_copy(c).start()

    def receive_core(j):
        core_copy(j).wait_recv()
        value, top, total = combine([w0[j, core], core_in[j]], half)
        with_meta((j,), works[0], value, top, total, half)
        for d in range(1, radices[0]):
            stage_copy(j, 0, d).start()

    def receive_stage(j, stage):
        for d in range(1, radices[stage]):
            stage_copy(j, stage, d).wait_recv()
        rows = stage_in[stage].shape[2]
        mine = works[stage][j, pl.ds(pl.multiple_of(digits[stage] * rows, rows), rows), :]
        value, top, total = combine(
            [mine] + [stage_in[stage][j, d - 1] for d in range(1, radices[stage])], half)
        if stage + 1 < stages:
            with_meta((j,), works[stage + 1], value, top, total, half)
            for d in range(1, radices[stage + 1]):
                stage_copy(j, stage + 1, d).start()
        else:
            gathered[j, core, first_piece(stage)] = (value / total).astype(jnp.bfloat16)
            for d in range(1, radices[stage]):
                gather_copy(j, stage, d).start()

    def receive_gather(j, stage):
        for d in range(1, radices[stage]):
            gather_arrival(j, stage, d).wait_recv()
        if stage:
            for d in range(1, radices[stage - 1]):
                gather_copy(j, stage - 1, d).start()
        else:
            core_gather(j, core).start()

    def finish(j):
        core_gather(j, 1 - core).wait_recv()
        for h in range(2):
            out_ref[pl.ds(pl.multiple_of(j * chunk, chunk), chunk), h * half:(h + 1) * half] = (
                gathered[j, h].reshape(chunk, half))
        core_copy(j).wait_send()
        for stage in range(stages):
            for d in range(1, radices[stage]):
                stage_copy(j, stage, d).wait_send()
                gather_copy(j, stage, d).wait_send()
        core_gather(j, core).wait_send()

    steps = [receive_core]
    steps += [functools.partial(receive_stage, stage=s) for s in range(stages)]
    steps += [functools.partial(receive_gather, stage=s) for s in reversed(range(stages))]
    steps += [finish]

    def iteration(i, carry):
        @pl.when(i < chunks)
        def _():
            @pl.when(lax.rem(i, per_request) == 0)
            def _():
                b = i // per_request
                load(b).wait()

                @pl.when(b + 1 < kv.shape[0])
                def _():
                    load(b + 1).start()

            compute(i)

        for lag in range(len(steps), 0, -1):
            j = i - lag

            @pl.when(jnp.logical_and(j >= 0, j < chunks))
            def _():
                steps[lag - 1](j)

        return carry

    lax.fori_loop(0, chunks + len(steps), iteration, 0)


def on_device(n, queries, latent_cache, lengths, offsets):
    requests, qtok, heads, width = queries.shape
    cache_dev = latent_cache.shape[1]
    rows = requests * qtok * heads
    radices = plan(n)
    stages = len(radices)
    chunk = max(2 * heads, n // 2 * 8)
    chunks = rows // chunk
    half = LATENT // 2
    wide = half + LANES
    works, stage_in, left = [], [], chunk
    for radix in radices:
        works.append(pltpu.VMEM((chunks, left, wide), jnp.float32))
        left //= radix
        stage_in.append(pltpu.VMEM((chunks, radix - 1, left, wide), jnp.float32))
    slots = 2 + 6 * stages
    out = pl.pallas_call(
        functools.partial(kernel, n, qtok, heads, chunk),
        out_shape=jax.ShapeDtypeStruct((rows, LATENT), jnp.bfloat16),
        in_specs=[
            pl.BlockSpec(memory_space=pltpu.SMEM),
            pl.BlockSpec(memory_space=pltpu.SMEM),
            pl.BlockSpec(memory_space=pltpu.VMEM),
            pl.BlockSpec(memory_space=pl.ANY),
        ],
        out_specs=pl.BlockSpec(memory_space=pltpu.VMEM),
        scratch_shapes=[
            pltpu.VMEM((requests, cache_dev, width), jnp.bfloat16),
            pltpu.VMEM((chunk, cache_dev), jnp.float32),
            pltpu.VMEM((chunks, 2, chunk, wide), jnp.float32),
            pltpu.VMEM((chunks, chunk, wide), jnp.float32),
            works,
            stage_in,
            pltpu.VMEM((chunks, 2, n // 2, chunk // (n // 2), half), jnp.bfloat16),
            pltpu.SemaphoreType.DMA((requests,)),
            pltpu.SemaphoreType.DMA((chunks, slots)),
            pltpu.SemaphoreType.DMA((chunks, slots)),
        ],
        compiler_params=pltpu.CompilerParams(
            collective_id=0, has_side_effects=True, vmem_limit_bytes=60 * 1024 * 1024),
        name="latent_attention",
    )(lengths, offsets, queries.reshape(rows, width), latent_cache)
    return out.reshape(requests, qtok, heads, LATENT)


def solution(mesh):
    placed = (P(), P(None, "seq", None), P(), P())
    body = functools.partial(on_device, mesh.shape["seq"])
    return jax.shard_map(body, mesh=mesh, in_specs=placed, out_specs=P(), check_vma=False)
```

```python
import functools

import jax
import jax.numpy as jnp
from jax import lax
from jax.experimental import pallas as pl
from jax.experimental.pallas import tpu as pltpu
from jax.sharding import PartitionSpec as P

LATENT = 512
LANES = 128
LOG2E = 1.4426950408889634
SCALE2 = (192.0 ** (-0.5)) * LOG2E
MESH = pl.DeviceIdType.MESH


def plan(n):
    chips, radices = n // 2, []
    while chips > 1:
        radix = 4 if chips % 4 == 0 else 2
        radices.append(radix)
        chips //= radix
    return radices


def split_meta(block, half):
    return block[:, :half], block[:, half:half + 1], block[:, half + 64:half + 65]


def with_meta(ref_index, ref, value, peak, total, half):
    rows = value.shape[0]
    lane = lax.broadcasted_iota(jnp.int32, (rows, LANES), 1)
    ref[(*ref_index, slice(None), pl.ds(0, half))] = value
    ref[(*ref_index, slice(None), pl.ds(half, LANES))] = jnp.where(lane < 64, peak, total)


def combine(blocks, half):
    parts = [split_meta(block, half) for block in blocks]
    top = functools.reduce(jnp.maximum, [p[1] for p in parts])
    factors = [jnp.exp2(p[1] - top) for p in parts]
    value = sum(p[0] * f for p, f in zip(parts, factors))
    total = sum(p[2] * f for p, f in zip(parts, factors))
    return value, top, total


def kernel(n, qtok, heads, chunk, lengths, offsets, q_ref, cache_hbm, out_ref,
           kv, score, w0, core_in, works, stage_in, gathered, load_sem, send_sem, recv_sem):
    rows_all = q_ref.shape[0] * heads
    cache_dev = kv.shape[2]
    half = LATENT // 2
    chunks = rows_all // chunk
    per_request = qtok * heads // chunk
    tokens = chunk // heads
    radices = plan(n)
    stages = len(radices)
    strides, blocks, pieces = [], [], n // 2
    stride, left = 1, pieces
    for radix in radices:
        strides.append(stride)
        stride *= radix
        left //= radix
        blocks.append(left)
    piece_rows = chunk // pieces

    me = lax.axis_index("seq")
    core = lax.rem(me, 2)
    chip = me // 2
    digits = [lax.rem(chip // s, r) for s, r in zip(strides, radices)]
    partner = me + 1 - 2 * core

    def peer(stage, d):
        other = lax.rem(digits[stage] + d, radices[stage])
        return other, me + (other - digits[stage]) * strides[stage] * 2

    barrier = pltpu.get_barrier_semaphore()
    peers = [partner]
    for stage in range(stages):
        peers += [peer(stage, d)[1] for d in range(1, radices[stage])]
    for device in peers:
        pl.semaphore_signal(barrier, inc=1, device_id=(device,), device_id_type=MESH)

    def load(b):
        return pltpu.make_async_copy(cache_hbm.at[b], kv.at[b], load_sem.at[b])

    load(0).start()
    pl.semaphore_wait(barrier, len(peers))

    start = me * cache_dev
    span = 512
    value_span = 1024

    def remote(src, dst, j, slot, device):
        return pltpu.make_async_remote_copy(
            src_ref=src, dst_ref=dst, send_sem=send_sem.at[j, slot],
            recv_sem=recv_sem.at[j, slot], device_id=(device,), device_id_type=MESH)

    def core_copy(j):
        return remote(w0.at[j, 1 - core], core_in.at[j], j, 0, partner)

    def stage_copy(j, stage, d):
        other, device = peer(stage, d)
        rows = chunk
        for r in radices[:stage + 1]:
            rows //= r
        src = works[stage].at[j, pl.ds(other * rows, rows)]
        return remote(src, stage_in[stage].at[j, d - 1], j, 1 + 3 * stage + d - 1, device)

    def first_piece(stage):
        return sum(digits[i] * blocks[i] for i in range(stage + 1))

    def gather_copy(j, stage, d):
        _, device = peer(stage, d)
        ref = gathered.at[j, core, pl.ds(first_piece(stage), blocks[stage])]
        return remote(ref, ref, j, 1 + 3 * stages + 3 * stage + d - 1, device)

    def gather_arrival(j, stage, d):
        _, device = peer(stage, d)
        origin = lax.rem(digits[stage] + radices[stage] - d, radices[stage])
        first = origin * blocks[stage]
        if stage:
            first = first + first_piece(stage - 1)
        ref = gathered.at[j, core, pl.ds(first, blocks[stage])]
        return remote(ref, ref, j, 1 + 3 * stages + 3 * stage + d - 1, device)

    def core_gather(j, which):
        ref = gathered.at[j, which]
        return remote(ref, ref, j, 1 + 6 * stages, partner)

    def compute(c):
        b = c // per_request
        first_token = lax.rem(c, per_request) * tokens
        limits = [lengths[b] - (qtok - 1) + offsets[b, first_token + t] - start for t in range(tokens)]
        q = jnp.concatenate([q_ref[c * tokens + t].T for t in range(tokens)], axis=0)
        peak = jnp.full((chunk, LANES), -1e30, jnp.float32)
        for j in range(cache_dev // span):
            s = jnp.dot(q, kv[b, :, j * span:(j + 1) * span], preferred_element_type=jnp.float32)
            places = lax.broadcasted_iota(jnp.int32, (heads, span), 1) + j * span
            s = jnp.concatenate(
                [jnp.where(places < limits[t], s[t * heads:(t + 1) * heads] * SCALE2, -1e30)
                 for t in range(tokens)], axis=0)
            score[:, j * span:(j + 1) * span] = s
            for i in range(span // LANES):
                peak = jnp.maximum(peak, s[:, i * LANES:(i + 1) * LANES])
        peak = jnp.max(peak, axis=1, keepdims=True)
        base = jnp.maximum(peak, -1e29)
        total = jnp.zeros((chunk, LANES), jnp.float32)
        value = jnp.zeros((chunk, LATENT), jnp.float32)
        for j in range(cache_dev // value_span):
            w = jnp.exp2(score[:, j * value_span:(j + 1) * value_span] - base)
            for i in range(value_span // LANES):
                total = total + w[:, i * LANES:(i + 1) * LANES]
            value = value + lax.dot_general(
                w.astype(jnp.bfloat16), kv[b, :LATENT, j * value_span:(j + 1) * value_span],
                (((1,), (1,)), ((), ())), preferred_element_type=jnp.float32)
        total = jnp.sum(total, axis=1, keepdims=True)
        for h in range(2):
            with_meta((c, h), w0, value[:, h * half:(h + 1) * half], peak, total, half)
        core_copy(c).start()

    def receive_core(j):
        core_copy(j).wait_recv()
        value, top, total = combine([w0[j, core], core_in[j]], half)
        with_meta((j,), works[0], value, top, total, half)
        for d in range(1, radices[0]):
            stage_copy(j, 0, d).start()

    def receive_stage(j, stage):
        for d in range(1, radices[stage]):
            stage_copy(j, stage, d).wait_recv()
        rows = stage_in[stage].shape[2]
        mine = works[stage][j, pl.ds(pl.multiple_of(digits[stage] * rows, rows), rows), :]
        value, top, total = combine(
            [mine] + [stage_in[stage][j, d - 1] for d in range(1, radices[stage])], half)
        if stage + 1 < stages:
            with_meta((j,), works[stage + 1], value, top, total, half)
            for d in range(1, radices[stage + 1]):
                stage_copy(j, stage + 1, d).start()
        else:
            gathered[j, core, first_piece(stage)] = (value / total).astype(jnp.bfloat16)
            for d in range(1, radices[stage]):
                gather_copy(j, stage, d).start()

    def receive_gather(j, stage):
        for d in range(1, radices[stage]):
            gather_arrival(j, stage, d).wait_recv()
        if stage:
            for d in range(1, radices[stage - 1]):
                gather_copy(j, stage - 1, d).start()
        else:
            core_gather(j, core).start()

    def finish(j):
        core_gather(j, 1 - core).wait_recv()
        for h in range(2):
            out_ref[pl.ds(pl.multiple_of(j * chunk, chunk), chunk), h * half:(h + 1) * half] = (
                gathered[j, h].reshape(chunk, half))
        core_copy(j).wait_send()
        for stage in range(stages):
            for d in range(1, radices[stage]):
                stage_copy(j, stage, d).wait_send()
                gather_copy(j, stage, d).wait_send()
        core_gather(j, core).wait_send()

    steps = [receive_core]
    steps += [functools.partial(receive_stage, stage=s) for s in range(stages)]
    steps += [functools.partial(receive_gather, stage=s) for s in reversed(range(stages))]
    steps += [finish]

    def iteration(i, carry):
        @pl.when(i < chunks)
        def _():
            @pl.when(lax.rem(i, per_request) == 0)
            def _():
                b = i // per_request
                load(b).wait()

                @pl.when(b + 1 < kv.shape[0])
                def _():
                    load(b + 1).start()

            compute(i)

        for lag in range(len(steps), 0, -1):
            j = i - lag

            @pl.when(jnp.logical_and(j >= 0, j < chunks))
            def _():
                steps[lag - 1](j)

        return carry

    lax.fori_loop(0, chunks + len(steps), iteration, 0)


def on_device(n, queries, latent_cache, lengths, offsets):
    requests, qtok, heads, width = queries.shape
    cache_dev = latent_cache.shape[1]
    rows = requests * qtok * heads
    radices = plan(n)
    stages = len(radices)
    chunk = max(2 * heads, n // 2 * 8)
    chunks = rows // chunk
    half = LATENT // 2
    wide = half + LANES
    works, stage_in, left = [], [], chunk
    for radix in radices:
        works.append(pltpu.VMEM((chunks, left, wide), jnp.float32))
        left //= radix
        stage_in.append(pltpu.VMEM((chunks, radix - 1, left, wide), jnp.float32))
    slots = 2 + 6 * stages
    out = pl.pallas_call(
        functools.partial(kernel, n, qtok, heads, chunk),
        out_shape=jax.ShapeDtypeStruct((rows, LATENT), jnp.bfloat16),
        in_specs=[
            pl.BlockSpec(memory_space=pltpu.SMEM),
            pl.BlockSpec(memory_space=pltpu.SMEM),
            pl.BlockSpec(memory_space=pltpu.VMEM),
            pl.BlockSpec(memory_space=pl.ANY),
        ],
        out_specs=pl.BlockSpec(memory_space=pltpu.VMEM),
        scratch_shapes=[
            pltpu.VMEM((requests, width, cache_dev), jnp.bfloat16),
            pltpu.VMEM((chunk, cache_dev), jnp.float32),
            pltpu.VMEM((chunks, 2, chunk, wide), jnp.float32),
            pltpu.VMEM((chunks, chunk, wide), jnp.float32),
            works,
            stage_in,
            pltpu.VMEM((chunks, 2, n // 2, chunk // (n // 2), half), jnp.bfloat16),
            pltpu.SemaphoreType.DMA((requests,)),
            pltpu.SemaphoreType.DMA((chunks, slots)),
            pltpu.SemaphoreType.DMA((chunks, slots)),
        ],
        compiler_params=pltpu.CompilerParams(
            collective_id=0, has_side_effects=True, vmem_limit_bytes=60 * 1024 * 1024),
        name="latent_attention",
    )(lengths, offsets, jnp.swapaxes(queries, 2, 3).reshape(requests * qtok, width, heads),
      jnp.swapaxes(latent_cache, 1, 2))
    return out.reshape(requests, qtok, heads, LATENT)


def solution(mesh):
    placed = (P(), P(None, "seq", None), P(), P())
    body = functools.partial(on_device, mesh.shape["seq"])
    return jax.shard_map(body, mesh=mesh, in_specs=placed, out_specs=P(), check_vma=False)
```

```python
import functools

import jax
import jax.numpy as jnp
from jax import lax
from jax.experimental import pallas as pl
from jax.experimental.pallas import tpu as pltpu
from jax.sharding import PartitionSpec as P

LATENT = 512
LANES = 128
LOG2E = 1.4426950408889634
SCALE2 = (192.0 ** (-0.5)) * LOG2E
MESH = pl.DeviceIdType.MESH


def plan(n):
    chips, radices = n // 2, []
    while chips > 1:
        radix = 4 if chips % 4 == 0 else 2
        radices.append(radix)
        chips //= radix
    return radices


def split_meta(block, half):
    return block[:, :half], block[:, half:half + 1], block[:, half + 64:half + 65]


def with_meta(ref_index, ref, value, peak, total, half):
    rows = value.shape[0]
    lane = lax.broadcasted_iota(jnp.int32, (rows, LANES), 1)
    ref[(*ref_index, slice(None), pl.ds(0, half))] = value
    ref[(*ref_index, slice(None), pl.ds(half, LANES))] = jnp.where(lane < 64, peak, total)


def combine(blocks, half):
    parts = [split_meta(block, half) for block in blocks]
    top = functools.reduce(jnp.maximum, [p[1] for p in parts])
    factors = [jnp.exp2(p[1] - top) for p in parts]
    value = sum(p[0] * f for p, f in zip(parts, factors))
    total = sum(p[2] * f for p, f in zip(parts, factors))
    return value, top, total


def kernel(n, qtok, heads, chunk, lengths, offsets, q_ref, cache_hbm, out_ref,
           kv, score, w0, core_in, works, stage_in, meta, meta_in, factors, gathered,
           load_sem, send_sem, recv_sem):
    rows_all = q_ref.shape[0] * heads
    cache_dev = kv.shape[2]
    half = LATENT // 2
    chunks = rows_all // chunk
    per_request = qtok * heads // chunk
    tokens = chunk // heads
    radices = plan(n)
    stages = len(radices)
    strides, blocks, pieces = [], [], n // 2
    stride, left = 1, pieces
    for radix in radices:
        strides.append(stride)
        stride *= radix
        left //= radix
        blocks.append(left)
    piece_rows = chunk // pieces

    me = lax.axis_index("seq")
    core = lax.rem(me, 2)
    chip = me // 2
    digits = [lax.rem(chip // s, r) for s, r in zip(strides, radices)]
    partner = me + 1 - 2 * core

    def peer(stage, d):
        other = lax.rem(digits[stage] + d, radices[stage])
        return other, me + (other - digits[stage]) * strides[stage] * 2

    barrier = pltpu.get_barrier_semaphore()
    peers = [partner]
    for stage in range(stages):
        peers += [peer(stage, d)[1] for d in range(1, radices[stage])]
    for device in peers:
        pl.semaphore_signal(barrier, inc=1, device_id=(device,), device_id_type=MESH)

    def load(b):
        return pltpu.make_async_copy(cache_hbm.at[b], kv.at[b], load_sem.at[b])

    load(0).start()
    pl.semaphore_wait(barrier, len(peers))

    start = me * cache_dev
    span = 512
    value_span = 1024

    def remote(src, dst, j, slot, device):
        return pltpu.make_async_remote_copy(
            src_ref=src, dst_ref=dst, send_sem=send_sem.at[j, slot],
            recv_sem=recv_sem.at[j, slot], device_id=(device,), device_id_type=MESH)

    def core_copy(j):
        return remote(w0.at[j, 1 - core], core_in.at[j], j, 0, partner)

    def stage_copy(j, stage, d):
        other, device = peer(stage, d)
        rows = chunk
        for r in radices[:stage + 1]:
            rows //= r
        src = works[stage].at[j, pl.ds(other * rows, rows)]
        return remote(src, stage_in[stage].at[j, d - 1], j, 1 + 3 * stage + d - 1, device)

    def meta_copy(j, stage, d):
        _, device = peer(stage, d)
        slot = 2 + 6 * stages + 3 * stage + d - 1
        return remote(meta[stage].at[j], meta_in[stage].at[j, d - 1], j, slot, device)

    def send_stage(j, stage):
        for d in range(1, radices[stage]):
            meta_copy(j, stage, d).start()
            stage_copy(j, stage, d).start()

    def pack(top, total):
        return jnp.where(lax.broadcasted_iota(jnp.int32, (8, chunk), 0) == 0, top, total)

    def first_piece(stage):
        return sum(digits[i] * blocks[i] for i in range(stage + 1))

    def gather_copy(j, stage, d):
        _, device = peer(stage, d)
        ref = gathered.at[j, core, pl.ds(first_piece(stage), blocks[stage])]
        return remote(ref, ref, j, 1 + 3 * stages + 3 * stage + d - 1, device)

    def gather_arrival(j, stage, d):
        _, device = peer(stage, d)
        origin = lax.rem(digits[stage] + radices[stage] - d, radices[stage])
        first = origin * blocks[stage]
        if stage:
            first = first + first_piece(stage - 1)
        ref = gathered.at[j, core, pl.ds(first, blocks[stage])]
        return remote(ref, ref, j, 1 + 3 * stages + 3 * stage + d - 1, device)

    def core_gather(j, which):
        ref = gathered.at[j, which]
        return remote(ref, ref, j, 1 + 6 * stages, partner)

    def compute(c):
        b = c // per_request
        first_token = lax.rem(c, per_request) * tokens
        limits = [lengths[b] - (qtok - 1) + offsets[b, first_token + t] - start for t in range(tokens)]
        q = jnp.concatenate([q_ref[c * tokens + t].T for t in range(tokens)], axis=0)
        peak = jnp.full((chunk, LANES), -1e30, jnp.float32)
        for j in range(cache_dev // span):
            s = jnp.dot(q, kv[b, :, j * span:(j + 1) * span], preferred_element_type=jnp.float32)
            places = lax.broadcasted_iota(jnp.int32, (heads, span), 1) + j * span
            s = jnp.concatenate(
                [jnp.where(places < limits[t], s[t * heads:(t + 1) * heads] * SCALE2, -1e30)
                 for t in range(tokens)], axis=0)
            score[:, j * span:(j + 1) * span] = s
            for i in range(span // LANES):
                peak = jnp.maximum(peak, s[:, i * LANES:(i + 1) * LANES])
        peak = jnp.max(peak, axis=1, keepdims=True)

        @pl.when(c >= 1)
        def _():
            receive_core(c - 1)

        base = jnp.maximum(peak, -1e29)
        total = jnp.zeros((chunk, LANES), jnp.float32)
        value = jnp.zeros((chunk, LATENT), jnp.float32)
        for j in range(cache_dev // value_span):
            w = jnp.exp2(score[:, j * value_span:(j + 1) * value_span] - base)
            for i in range(value_span // LANES):
                total = total + w[:, i * LANES:(i + 1) * LANES]
            value = value + lax.dot_general(
                w.astype(jnp.bfloat16), kv[b, :LATENT, j * value_span:(j + 1) * value_span],
                (((1,), (1,)), ((), ())), preferred_element_type=jnp.float32)
        total = jnp.sum(total, axis=1, keepdims=True)
        for h in range(2):
            with_meta((c, h), w0, value[:, h * half:(h + 1) * half], peak, total, half)
        core_copy(c).start()

    def receive_core(j):
        core_copy(j).wait_recv()
        value, top, total = combine([w0[j, core], core_in[j]], half)
        works[0][j] = value
        lane = lax.broadcasted_iota(jnp.int32, (chunk, LANES), 1)
        turned = jnp.where(lane < 64, top, total).T
        meta[0][j] = pack(turned[:8], turned[64:72])
        send_stage(j, 0)

    def receive_stage(j, stage):
        radix = radices[stage]
        for d in range(1, radix):
            meta_copy(j, stage, d).wait_recv()
        metas = [meta[stage][j]] + [meta_in[stage][j, d - 1] for d in range(1, radix)]
        top = functools.reduce(jnp.maximum, [m[0:1] for m in metas])
        shares = [jnp.exp2(m[0:1] - top) for m in metas]
        total = sum(m[1:2] * f for m, f in zip(metas, shares))
        if stage + 1 == stages:
            shares = [f / total for f in shares]
        segment = LANES // radix
        factors[...] = jnp.concatenate(
            [jnp.broadcast_to(f, (segment, chunk)) for f in shares], axis=0).T
        rows = stage_in[stage].shape[2]
        first = pl.multiple_of(first_piece(stage) * piece_rows, piece_rows)
        mine = factors[pl.ds(first, rows), :]
        value = works[stage][j, pl.ds(pl.multiple_of(digits[stage] * rows, rows), rows), :] * mine[:, 0:1]
        for d in range(1, radix):
            stage_copy(j, stage, d).wait_recv()
            value = value + stage_in[stage][j, d - 1] * mine[:, d * segment:d * segment + 1]
        if stage + 1 < stages:
            works[stage + 1][j] = value
            meta[stage + 1][j] = pack(top, total)
            send_stage(j, stage + 1)
        else:
            gathered[j, core, first_piece(stage)] = value.astype(jnp.bfloat16)
            for d in range(1, radix):
                gather_copy(j, stage, d).start()

    def receive_gather(j, stage):
        for d in range(1, radices[stage]):
            gather_arrival(j, stage, d).wait_recv()
        if stage:
            for d in range(1, radices[stage - 1]):
                gather_copy(j, stage - 1, d).start()
        else:
            core_gather(j, core).start()

    def finish(j):
        core_gather(j, 1 - core).wait_recv()
        for h in range(2):
            out_ref[pl.ds(pl.multiple_of(j * chunk, chunk), chunk), h * half:(h + 1) * half] = (
                gathered[j, h].reshape(chunk, half))
        core_copy(j).wait_send()
        for stage in range(stages):
            for d in range(1, radices[stage]):
                stage_copy(j, stage, d).wait_send()
                meta_copy(j, stage, d).wait_send()
                gather_copy(j, stage, d).wait_send()
        core_gather(j, core).wait_send()

    steps = [functools.partial(receive_stage, stage=s) for s in range(stages)]
    steps += [functools.partial(receive_gather, stage=s) for s in reversed(range(stages))]
    steps += [finish]

    def iteration(i, carry):
        @pl.when(i < chunks)
        def _():
            @pl.when(lax.rem(i, per_request) == 0)
            def _():
                b = i // per_request
                load(b).wait()

                @pl.when(b + 1 < kv.shape[0])
                def _():
                    load(b + 1).start()

            compute(i)

        @pl.when(i == chunks)
        def _():
            receive_core(chunks - 1)

        for lag, step in enumerate(steps, 3):
            j = i - lag

            @pl.when(jnp.logical_and(j >= 0, j < chunks))
            def _():
                step(j)

        return carry

    lax.fori_loop(0, chunks + len(steps) + 2, iteration, 0)


def on_device(n, queries, latent_cache, lengths, offsets):
    requests, qtok, heads, width = queries.shape
    cache_dev = latent_cache.shape[1]
    rows = requests * qtok * heads
    radices = plan(n)
    stages = len(radices)
    chunk = max(2 * heads, n // 2 * 8)
    chunks = rows // chunk
    half = LATENT // 2
    wide = half + LANES
    works, stage_in, meta, meta_in, left = [], [], [], [], chunk
    for radix in radices:
        works.append(pltpu.VMEM((chunks, left, half), jnp.float32))
        left //= radix
        stage_in.append(pltpu.VMEM((chunks, radix - 1, left, half), jnp.float32))
        meta.append(pltpu.VMEM((chunks, 8, chunk), jnp.float32))
        meta_in.append(pltpu.VMEM((chunks, radix - 1, 8, chunk), jnp.float32))
    slots = 2 + 9 * stages
    out = pl.pallas_call(
        functools.partial(kernel, n, qtok, heads, chunk),
        out_shape=jax.ShapeDtypeStruct((rows, LATENT), jnp.bfloat16),
        in_specs=[
            pl.BlockSpec(memory_space=pltpu.SMEM),
            pl.BlockSpec(memory_space=pltpu.SMEM),
            pl.BlockSpec(memory_space=pltpu.VMEM),
            pl.BlockSpec(memory_space=pl.ANY),
        ],
        out_specs=pl.BlockSpec(memory_space=pltpu.VMEM),
        scratch_shapes=[
            pltpu.VMEM((requests, width, cache_dev), jnp.bfloat16),
            pltpu.VMEM((chunk, cache_dev), jnp.float32),
            pltpu.VMEM((chunks, 2, chunk, wide), jnp.float32),
            pltpu.VMEM((chunks, chunk, wide), jnp.float32),
            works,
            stage_in,
            meta,
            meta_in,
            pltpu.VMEM((chunk, LANES), jnp.float32),
            pltpu.VMEM((chunks, 2, n // 2, chunk // (n // 2), half), jnp.bfloat16),
            pltpu.SemaphoreType.DMA((requests,)),
            pltpu.SemaphoreType.DMA((chunks, slots)),
            pltpu.SemaphoreType.DMA((chunks, slots)),
        ],
        compiler_params=pltpu.CompilerParams(
            collective_id=0, has_side_effects=True, vmem_limit_bytes=60 * 1024 * 1024),
        name="latent_attention",
    )(lengths, offsets, jnp.swapaxes(queries, 2, 3).reshape(requests * qtok, width, heads),
      jnp.swapaxes(latent_cache, 1, 2))
    return out.reshape(requests, qtok, heads, LATENT)


def solution(mesh):
    placed = (P(), P(None, "seq", None), P(), P())
    body = functools.partial(on_device, mesh.shape["seq"])
    return jax.shard_map(body, mesh=mesh, in_specs=placed, out_specs=P(), check_vma=False)
```

```python
import functools

import jax
import jax.numpy as jnp
from jax import lax
from jax.experimental import pallas as pl
from jax.experimental.pallas import tpu as pltpu
from jax.sharding import PartitionSpec as P

LATENT = 512
LANES = 128
LOG2E = 1.4426950408889634
SCALE2 = (192.0 ** (-0.5)) * LOG2E
MESH = pl.DeviceIdType.MESH


def plan(n):
    chips, radices = n // 2, []
    while chips > 1:
        radix = 4 if chips % 4 == 0 else 2
        radices.append(radix)
        chips //= radix
    return radices


def split_meta(block, half):
    return block[:, :half], block[:, half:half + 1], block[:, half + 64:half + 65]


def with_meta(ref_index, ref, value, peak, total, half):
    rows = value.shape[0]
    lane = lax.broadcasted_iota(jnp.int32, (rows, LANES), 1)
    ref[(*ref_index, slice(None), pl.ds(0, half))] = value
    ref[(*ref_index, slice(None), pl.ds(half, LANES))] = jnp.where(lane < 64, peak, total)


def combine(blocks, half):
    parts = [split_meta(block, half) for block in blocks]
    top = functools.reduce(jnp.maximum, [p[1] for p in parts])
    factors = [jnp.exp2(p[1] - top) for p in parts]
    value = sum(p[0] * f for p, f in zip(parts, factors))
    total = sum(p[2] * f for p, f in zip(parts, factors))
    return value, top, total


def kernel(n, qtok, heads, chunk, lengths, offsets, q_ref, cache_hbm, out_ref,
           kv, score, w0, core_in, works, stage_in, meta, meta_in, factors, gathered,
           load_sem, send_sem, recv_sem):
    rows_all = q_ref.shape[0] * heads
    cache_dev = kv.shape[2]
    half = LATENT // 2
    chunks = rows_all // chunk
    per_request = qtok * heads // chunk
    tokens = chunk // heads
    radices = plan(n)
    stages = len(radices)
    strides, blocks, pieces = [], [], n // 2
    stride, left = 1, pieces
    for radix in radices:
        strides.append(stride)
        stride *= radix
        left //= radix
        blocks.append(left)
    piece_rows = chunk // pieces

    me = lax.axis_index("seq")
    core = lax.rem(me, 2)
    chip = me // 2
    digits = [lax.rem(chip // s, r) for s, r in zip(strides, radices)]
    partner = me + 1 - 2 * core

    even = len(set(radices)) == 1

    def turned_order(j, values, stage):
        if not even:
            return values[stage]
        swap = lax.rem(j, 2) * (1 - j // 2)
        return values[stage] + swap * (values[stages - 1 - stage] - values[stage])

    def digit(j, stage):
        return turned_order(j, digits, stage)

    def peer(j, stage, d):
        mine = digit(j, stage)
        other = lax.rem(mine + d, radices[stage])
        return other, me + (other - mine) * turned_order(j, strides, stage) * 2

    barrier = pltpu.get_barrier_semaphore()
    peers = [partner]
    for stage in range(stages):
        peers += [peer(0, stage, d)[1] for d in range(1, radices[stage])]
    for device in peers:
        pl.semaphore_signal(barrier, inc=1, device_id=(device,), device_id_type=MESH)

    load_parts = 4
    load_span = cache_dev // load_parts

    def load(b, part):
        where = (b, slice(None), pl.ds(part * load_span, load_span))
        return pltpu.make_async_copy(cache_hbm.at[where], kv.at[where], load_sem.at[b, part])

    for part in range(load_parts):
        load(0, part).start()
    pl.semaphore_wait(barrier, len(peers))

    start = me * cache_dev
    span = 512
    value_span = 1024

    def remote(src, dst, j, slot, device):
        return pltpu.make_async_remote_copy(
            src_ref=src, dst_ref=dst, send_sem=send_sem.at[j, slot],
            recv_sem=recv_sem.at[j, slot], device_id=(device,), device_id_type=MESH)

    def core_copy(j):
        return remote(w0.at[j, 1 - core], core_in.at[j], j, 0, partner)

    def stage_copy(j, stage, d):
        other, device = peer(j, stage, d)
        rows = chunk
        for r in radices[:stage + 1]:
            rows //= r
        src = works[stage].at[j, pl.ds(other * rows, rows)]
        return remote(src, stage_in[stage].at[j, d - 1], j, 1 + 3 * stage + d - 1, device)

    def meta_copy(j, stage, d):
        _, device = peer(j, stage, d)
        slot = 2 + 6 * stages + 3 * stage + d - 1
        return remote(meta[stage].at[j], meta_in[stage].at[j, d - 1], j, slot, device)

    def send_stage(j, stage):
        for d in range(1, radices[stage]):
            meta_copy(j, stage, d).start()
            stage_copy(j, stage, d).start()

    def pack(top, total):
        return jnp.where(lax.broadcasted_iota(jnp.int32, (8, chunk), 0) == 0, top, total)

    def first_piece(j, stage):
        return sum(digit(j, i) * blocks[i] for i in range(stage + 1))

    def gather_copy(j, stage, d):
        _, device = peer(j, stage, d)
        ref = gathered.at[j, core, pl.ds(first_piece(j, stage), blocks[stage])]
        return remote(ref, ref, j, 1 + 3 * stages + 3 * stage + d - 1, device)

    def gather_arrival(j, stage, d):
        _, device = peer(j, stage, d)
        origin = lax.rem(digit(j, stage) + radices[stage] - d, radices[stage])
        first = origin * blocks[stage]
        if stage:
            first = first + first_piece(j, stage - 1)
        ref = gathered.at[j, core, pl.ds(first, blocks[stage])]
        return remote(ref, ref, j, 1 + 3 * stages + 3 * stage + d - 1, device)

    def core_gather(j, which):
        ref = gathered.at[j, which]
        return remote(ref, ref, j, 1 + 6 * stages, partner)

    def compute(c):
        b = c // per_request
        first_token = lax.rem(c, per_request) * tokens
        limits = [lengths[b] - (qtok - 1) + offsets[b, first_token + t] - start for t in range(tokens)]
        q = jnp.concatenate([q_ref[c * tokens + t].T for t in range(tokens)], axis=0)
        peak = jnp.full((chunk, LANES), -1e30, jnp.float32)
        fresh = lax.rem(c, per_request) == 0
        for j in range(cache_dev // span):
            if j * span % load_span == 0:
                @pl.when(fresh)
                def _():
                    load(b, j * span // load_span).wait()

            s = jnp.dot(q, kv[b, :, j * span:(j + 1) * span], preferred_element_type=jnp.float32)
            places = lax.broadcasted_iota(jnp.int32, (heads, span), 1) + j * span
            s = jnp.concatenate(
                [jnp.where(places < limits[t], s[t * heads:(t + 1) * heads] * SCALE2, -1e30)
                 for t in range(tokens)], axis=0)
            score[:, j * span:(j + 1) * span] = s
            for i in range(span // LANES):
                peak = jnp.maximum(peak, s[:, i * LANES:(i + 1) * LANES])
        peak = jnp.max(peak, axis=1, keepdims=True)

        @pl.when(jnp.logical_and(fresh, b + 1 < kv.shape[0]))
        def _():
            for part in range(load_parts):
                load(b + 1, part).start()

        @pl.when(c >= 1)
        def _():
            receive_core(c - 1)

        base = jnp.maximum(peak, -1e29)
        total = jnp.zeros((chunk, LANES), jnp.float32)
        value = jnp.zeros((chunk, LATENT), jnp.float32)
        for j in range(cache_dev // value_span):
            w = jnp.exp2(score[:, j * value_span:(j + 1) * value_span] - base)
            for i in range(value_span // LANES):
                total = total + w[:, i * LANES:(i + 1) * LANES]
            value = value + lax.dot_general(
                w.astype(jnp.bfloat16), kv[b, :LATENT, j * value_span:(j + 1) * value_span],
                (((1,), (1,)), ((), ())), preferred_element_type=jnp.float32)
        total = jnp.sum(total, axis=1, keepdims=True)
        for h in range(2):
            with_meta((c, h), w0, value[:, h * half:(h + 1) * half], peak, total, half)
        core_copy(c).start()

    def receive_core(j):
        core_copy(j).wait_recv()
        value, top, total = combine([w0[j, core], core_in[j]], half)
        works[0][j] = value
        lane = lax.broadcasted_iota(jnp.int32, (chunk, LANES), 1)
        turned = jnp.where(lane < 64, top, total).T
        meta[0][j] = pack(turned[:8], turned[64:72])
        send_stage(j, 0)

    def receive_stage(j, stage):
        radix = radices[stage]
        for d in range(1, radix):
            meta_copy(j, stage, d).wait_recv()
        metas = [meta[stage][j]] + [meta_in[stage][j, d - 1] for d in range(1, radix)]
        top = functools.reduce(jnp.maximum, [m[0:1] for m in metas])
        shares = [jnp.exp2(m[0:1] - top) for m in metas]
        total = sum(m[1:2] * f for m, f in zip(metas, shares))
        if stage + 1 == stages:
            shares = [f / total for f in shares]
        segment = LANES // radix
        factors[...] = jnp.concatenate(
            [jnp.broadcast_to(f, (segment, chunk)) for f in shares], axis=0).T
        rows = stage_in[stage].shape[2]
        first = pl.multiple_of(first_piece(j, stage) * piece_rows, piece_rows)
        mine = factors[pl.ds(first, rows), :]
        value = works[stage][j, pl.ds(pl.multiple_of(digit(j, stage) * rows, rows), rows), :] * mine[:, 0:1]
        for d in range(1, radix):
            stage_copy(j, stage, d).wait_recv()
            value = value + stage_in[stage][j, d - 1] * mine[:, d * segment:d * segment + 1]
        if stage + 1 < stages:
            works[stage + 1][j] = value
            meta[stage + 1][j] = pack(top, total)
            send_stage(j, stage + 1)
        else:
            gathered[j, core, first_piece(j, stage)] = value.astype(jnp.bfloat16)
            for d in range(1, radix):
                gather_copy(j, stage, d).start()

    def receive_gather(j, stage):
        for d in range(1, radices[stage]):
            gather_arrival(j, stage, d).wait_recv()
        if stage:
            for d in range(1, radices[stage - 1]):
                gather_copy(j, stage - 1, d).start()
        else:
            core_gather(j, core).start()

    def finish(j):
        core_gather(j, 1 - core).wait_recv()
        for h in range(2):
            out_ref[pl.ds(pl.multiple_of(j * chunk, chunk), chunk), h * half:(h + 1) * half] = (
                gathered[j, h].reshape(chunk, half))
        core_copy(j).wait_send()
        for stage in range(stages):
            for d in range(1, radices[stage]):
                stage_copy(j, stage, d).wait_send()
                meta_copy(j, stage, d).wait_send()
                gather_copy(j, stage, d).wait_send()
        core_gather(j, core).wait_send()

    steps = [functools.partial(receive_stage, stage=s) for s in range(stages)]
    steps += [functools.partial(receive_gather, stage=s) for s in reversed(range(stages))]
    steps += [finish]

    def iteration(i, carry):
        @pl.when(i < chunks)
        def _():
            compute(i)

        @pl.when(i == chunks)
        def _():
            receive_core(chunks - 1)

        for lag, step in enumerate(steps, 3):
            j = i - lag

            @pl.when(jnp.logical_and(j >= 0, j < chunks))
            def _():
                step(j)

        return carry

    lax.fori_loop(0, chunks + len(steps) + 2, iteration, 0)


def on_device(n, queries, latent_cache, lengths, offsets):
    requests, qtok, heads, width = queries.shape
    cache_dev = latent_cache.shape[1]
    rows = requests * qtok * heads
    radices = plan(n)
    stages = len(radices)
    chunk = max(2 * heads, n // 2 * 8)
    chunks = rows // chunk
    half = LATENT // 2
    wide = half + LANES
    works, stage_in, meta, meta_in, left = [], [], [], [], chunk
    for radix in radices:
        works.append(pltpu.VMEM((chunks, left, half), jnp.float32))
        left //= radix
        stage_in.append(pltpu.VMEM((chunks, radix - 1, left, half), jnp.float32))
        meta.append(pltpu.VMEM((chunks, 8, chunk), jnp.float32))
        meta_in.append(pltpu.VMEM((chunks, radix - 1, 8, chunk), jnp.float32))
    slots = 2 + 9 * stages
    out = pl.pallas_call(
        functools.partial(kernel, n, qtok, heads, chunk),
        out_shape=jax.ShapeDtypeStruct((rows, LATENT), jnp.bfloat16),
        in_specs=[
            pl.BlockSpec(memory_space=pltpu.SMEM),
            pl.BlockSpec(memory_space=pltpu.SMEM),
            pl.BlockSpec(memory_space=pltpu.VMEM),
            pl.BlockSpec(memory_space=pl.ANY),
        ],
        out_specs=pl.BlockSpec(memory_space=pltpu.VMEM),
        scratch_shapes=[
            pltpu.VMEM((requests, width, cache_dev), jnp.bfloat16),
            pltpu.VMEM((chunk, cache_dev), jnp.float32),
            pltpu.VMEM((chunks, 2, chunk, wide), jnp.float32),
            pltpu.VMEM((chunks, chunk, wide), jnp.float32),
            works,
            stage_in,
            meta,
            meta_in,
            pltpu.VMEM((chunk, LANES), jnp.float32),
            pltpu.VMEM((chunks, 2, n // 2, chunk // (n // 2), half), jnp.bfloat16),
            pltpu.SemaphoreType.DMA((requests, 4)),
            pltpu.SemaphoreType.DMA((chunks, slots)),
            pltpu.SemaphoreType.DMA((chunks, slots)),
        ],
        compiler_params=pltpu.CompilerParams(
            collective_id=0, has_side_effects=True, vmem_limit_bytes=60 * 1024 * 1024),
        name="latent_attention",
    )(lengths, offsets, jnp.swapaxes(queries, 2, 3).reshape(requests * qtok, width, heads),
      jnp.swapaxes(latent_cache, 1, 2))
    return out.reshape(requests, qtok, heads, LATENT)


def solution(mesh):
    placed = (P(), P(None, "seq", None), P(), P())
    body = functools.partial(on_device, mesh.shape["seq"])
    return jax.shard_map(body, mesh=mesh, in_specs=placed, out_specs=P(), check_vma=False)
```
